32 devices in a mesh: dp: 8 (over z, core), mp: 4 (over y, x).
Axes of the slice: x: 2, y: 2, z: 4, core: 2. Of those that a mesh axis runs over, the one named last changes fastest.
Arguments:
- block_input: bfloat16 [4096, 6144], P('dp', 'mp'), may hold values from -6 to 6
- prenorm_gain: float32 [6144], P('mp'), may hold values from 0.5 to 1.5
- weight: bfloat16 [6144, 3072], P('mp', 'dp'), may hold values from -0.078125 to 0.078125
- query: bfloat16 [4096, 3072], P('dp'), may hold values from -6 to 6
- grad_normed: bfloat16 [4096, 3072], P('dp'), may hold values from -6 to 6
- qk_gain: float32 [128], replicated, may hold values from 0.5 to 1.5
Outputs:
- input_gradient: bfloat16 [4096, 6144], P('dp', 'mp')
- grad_weight: float32 [6144, 3072], P('mp', 'dp')
- prenorm_gain_gradient: float32 [6144], P('mp')
- grad_qk_gain: float32 [128], replicated
The draws below stay inside these ranges and needn't reach their ends.
All inputs are finite; a program needn't handle non-finite values.
Results may differ from the reference program's by a relative error of at most 0.0049.
Values may be sent and summed in bfloat16 or wider, within the bound.
A program may use at most 128 MiB of HBM per device.

```python
import jax
import jax.numpy as jnp
from jax import lax

D = 6144
HEADS = 24
HEAD_DIM = 128
WIDTH = 3072
TOKENS = 4096


def level_of(rng, shape, shards, low, largest):
    gain = 1.0
    for axis_at, blocks in shards:
        steps = jax.random.uniform(jax.random.fold_in(jax.random.fold_in(rng, 6), axis_at), (blocks,), jnp.float32, low / len(shards), largest / len(shards))
        gain = gain * jnp.repeat(jnp.exp(steps), shape[axis_at] // blocks).reshape((-1,) + (1,) * (len(shape) - 1 - axis_at))
    return gain


def centred(rng, dims, width, limit, cuts=(), kind=jnp.bfloat16):
    entries = width * jax.random.normal(rng, dims, jnp.float32)
    if cuts:
        entries = entries * level_of(rng, dims, cuts, -0.22, 0.18)
    return jnp.clip(entries, -limit, limit).astype(kind)


def setup_inputs(seed: int = 0) -> dict:
    splits = jax.random.split(jax.random.key(seed), 7)
    block_input = centred(splits[0], (TOKENS, D), 1.0, 6.0, ((0, 8), (1, 4)))
    prenorm_gain = jnp.clip(1.0 + 0.1 * jax.random.normal(splits[1], (D,), jnp.float32), 0.5, 1.5)
    weight = centred(splits[2], (D, WIDTH), D ** -0.5, 0.078125, ((0, 4), (1, 8)))
    query = centred(splits[3], (TOKENS, WIDTH), 1.0, 6.0, ((0, 8),))
    grad_normed = centred(splits[4], (TOKENS, WIDTH), 1.0, 6.0, ((0, 8),))
    qk_gain = jnp.clip(1.0 + 0.1 * jax.random.normal(splits[5], (HEAD_DIM,), jnp.float32), 0.5, 1.5)
    return {"block_input": block_input, "prenorm_gain": prenorm_gain, "weight": weight, "query": query, "grad_normed": grad_normed, "qk_gain": qk_gain}


EPS = 1e-06

def reference(block_input, prenorm_gain, weight, query, grad_normed, qk_gain):
    input_wide_float = block_input.astype(jnp.float32)
    row_average = lax.optimization_barrier(jnp.mean(input_wide_float, axis=1, keepdims=True))
    variance = lax.optimization_barrier(jnp.mean(input_wide_float * input_wide_float, axis=1, keepdims=True)) - row_average * row_average
    reciprocal_deviation = lax.rsqrt(variance + EPS)
    standardized_input = (input_wide_float - row_average) * reciprocal_deviation
    prenormed_rows = (standardized_input * prenorm_gain).astype(jnp.bfloat16)
    q_float = query.astype(jnp.float32).reshape(TOKENS, HEADS, HEAD_DIM)
    q_mean = lax.optimization_barrier(jnp.mean(q_float, axis=2, keepdims=True))
    q_var = lax.optimization_barrier(jnp.mean(q_float * q_float, axis=2, keepdims=True)) - q_mean * q_mean
    q_inv = lax.rsqrt(q_var + EPS)
    qhat = (q_float - q_mean) * q_inv
    upstream = grad_normed.astype(jnp.float32).reshape(TOKENS, HEADS, HEAD_DIM)
    dqhat = upstream * qk_gain
    grad_query = q_inv * (dqhat - lax.optimization_barrier(jnp.mean(dqhat, axis=2, keepdims=True)) - qhat * lax.optimization_barrier(jnp.mean(dqhat * qhat, axis=2, keepdims=True)))
    grad_query = grad_query.reshape(TOKENS, WIDTH).astype(jnp.bfloat16)
    grad_qk_gain = lax.optimization_barrier(jnp.sum(upstream * qhat, axis=(0, 1)))
    grad_weight = jnp.dot(prenormed_rows.T, grad_query, preferred_element_type=jnp.float32)
    gradient_prenormed_input = jnp.dot(grad_query, weight.T, preferred_element_type=jnp.float32)
    prenorm_gain_gradient = lax.optimization_barrier(jnp.sum(gradient_prenormed_input * standardized_input, axis=0))
    standardized_gradient = gradient_prenormed_input * prenorm_gain
    input_gradient = reciprocal_deviation * (standardized_gradient - lax.optimization_barrier(jnp.mean(standardized_gradient, axis=1, keepdims=True)) - standardized_input * lax.optimization_barrier(jnp.mean(standardized_gradient * standardized_input, axis=1, keepdims=True)))
    return (input_gradient.astype(jnp.bfloat16), grad_weight, prenorm_gain_gradient, grad_qk_gain)
```

```python
import jax
import jax.numpy as jnp
from jax import lax
from jax.experimental import pallas as pl
from jax.experimental.pallas import tpu as pltpu
from jax.sharding import PartitionSpec as P

D = 6144


EPS = 1e-06


def qk_kernel(query_ref, grad_ref, gain_ref, out_ref, contrib_ref):
    @pl.when(pl.program_id(0) == 0)
    def _():
        contrib_ref[...] = jnp.zeros_like(contrib_ref)

    head_size = gain_ref.shape[1]
    gain = gain_ref[...]
    total = jnp.zeros_like(contrib_ref)
    for head in range(query_ref.shape[1] // head_size):
        columns = pl.ds(head * head_size, head_size)
        q_float = query_ref[:, columns].astype(jnp.float32)
        upstream = grad_ref[:, columns].astype(jnp.float32)
        q_mean = jnp.mean(q_float, axis=1, keepdims=True)
        q_var = jnp.mean(q_float * q_float, axis=1, keepdims=True) - q_mean * q_mean
        q_inv = lax.rsqrt(q_var + EPS)
        qhat = (q_float - q_mean) * q_inv
        dqhat = upstream * gain
        dq_mean = jnp.mean(dqhat, axis=1, keepdims=True)
        dq_cross = jnp.mean(dqhat * qhat, axis=1, keepdims=True)
        out_ref[:, columns] = (q_inv * (dqhat - dq_mean - qhat * dq_cross)).astype(out_ref.dtype)
        product = upstream * qhat
        total += jnp.sum(product.reshape(-1, 8, head_size), axis=0)
    contrib_ref[...] += total


def qk_backward(query, grad_normed, qk_gain):
    rows, width = query.shape
    head_size = qk_gain.shape[0]
    block = min(rows, 64)
    grad_query, contrib = pl.pallas_call(
        qk_kernel,
        grid=(rows // block,),
        in_specs=[
            pl.BlockSpec((block, width), lambda i: (i, 0)),
            pl.BlockSpec((block, width), lambda i: (i, 0)),
            pl.BlockSpec((1, head_size), lambda i: (0, 0)),
        ],
        out_specs=[
            pl.BlockSpec((block, width), lambda i: (i, 0)),
            pl.BlockSpec((8, head_size), lambda i: (0, 0)),
        ],
        out_shape=[
            jax.ShapeDtypeStruct((rows, width), jnp.bfloat16),
            jax.ShapeDtypeStruct((8, head_size), jnp.float32),
        ],
        compiler_params=pltpu.CompilerParams(vmem_limit_bytes=32 * 1024 * 1024),
        cost_estimate=pl.CostEstimate(flops=40 * rows * width, bytes_accessed=6 * rows * width, transcendentals=0),
    )(query, grad_normed, qk_gain.reshape(1, -1))
    return grad_query, jnp.sum(contrib, axis=0)


def shards(block_input, prenorm_gain, weight, query, grad_normed, qk_gain):
    input_wide_float = block_input.astype(jnp.float32)
    local_sum = jnp.sum(input_wide_float, axis=1)
    local_square = jnp.sum(input_wide_float * input_wide_float, axis=1)
    grad_query, qk_partial = qk_backward(query, grad_normed, qk_gain)
    gradient_prenormed_input = lax.dot_general(
        grad_query,
        lax.all_gather(weight, "dp", axis=1, tiled=True),
        (((1,), (1,)), ((), ())),
        preferred_element_type=jnp.float32,
    )
    standardized_gradient = gradient_prenormed_input * prenorm_gain
    total_sum, total_square = lax.psum((local_sum, local_square), "mp")
    row_average = (total_sum / D)[:, None]
    reciprocal_deviation = lax.rsqrt((total_square / D)[:, None] - row_average * row_average + EPS)
    standardized_input = (input_wide_float - row_average) * reciprocal_deviation
    slope_mean, slope_cross = lax.psum(
        (
            jnp.sum(standardized_gradient, axis=1),
            jnp.sum(standardized_gradient * standardized_input, axis=1),
        ),
        "mp",
    )
    average_standardized_gradient = (slope_mean / D)[:, None]
    average_cross_term = (slope_cross / D)[:, None]
    prenormed_rows = (standardized_input * prenorm_gain).astype(jnp.bfloat16)
    input_gradient = (
        reciprocal_deviation
        * (
            standardized_gradient
            - average_standardized_gradient
            - standardized_input * average_cross_term
        )
    ).astype(jnp.bfloat16)
    prenorm_gain_partial = jnp.sum(gradient_prenormed_input * standardized_input, axis=0)
    weight_partial = lax.dot_general(
        prenormed_rows, grad_query, (((0,), (0,)), ((), ())), preferred_element_type=jnp.float32
    )
    grad_weight = lax.psum_scatter(
        weight_partial.astype(jnp.bfloat16), "dp", scatter_dimension=1, tiled=True
    ).astype(jnp.float32)
    prenorm_gain_gradient, grad_qk_gain = lax.psum((prenorm_gain_partial, qk_partial), "dp")
    return (input_gradient, grad_weight, prenorm_gain_gradient, grad_qk_gain)


def solution(mesh):
    return jax.shard_map(
        shards,
        mesh=mesh,
        in_specs=(P("dp", "mp"), P("mp"), P("mp", "dp"), P("dp", None), P("dp", None), P()),
        out_specs=(P("dp", "mp"), P("mp", "dp"), P("mp"), P()),
        check_vma=False,
    )
```

```python
import math

import jax
import jax.numpy as jnp
from jax import lax
from jax.experimental import pallas as pl
from jax.experimental.pallas import tpu as pltpu
from jax.sharding import PartitionSpec as P

D = 6144


EPS = 1e-06


def qk_kernel(query_ref, grad_ref, gain_ref, out_ref, contrib_ref):
    @pl.when(pl.program_id(0) == 0)
    def _():
        contrib_ref[...] = jnp.zeros_like(contrib_ref)

    head_size = gain_ref.shape[1]
    gain = gain_ref[...]
    total = jnp.zeros_like(contrib_ref)
    for head in range(query_ref.shape[1] // head_size):
        columns = pl.ds(head * head_size, head_size)
        q_float = query_ref[:, columns].astype(jnp.float32)
        upstream = grad_ref[:, columns].astype(jnp.float32)
        q_mean = jnp.mean(q_float, axis=1, keepdims=True)
        q_var = jnp.mean(q_float * q_float, axis=1, keepdims=True) - q_mean * q_mean
        q_inv = lax.rsqrt(q_var + EPS)
        qhat = (q_float - q_mean) * q_inv
        dqhat = upstream * gain
        dq_mean = jnp.mean(dqhat, axis=1, keepdims=True)
        dq_cross = jnp.mean(dqhat * qhat, axis=1, keepdims=True)
        out_ref[:, columns] = (q_inv * (dqhat - dq_mean - qhat * dq_cross)).astype(out_ref.dtype)
        product = upstream * qhat
        total += jnp.sum(product.reshape(-1, 8, head_size), axis=0)
    contrib_ref[...] += total


def qk_backward(query, grad_normed, qk_gain):
    rows, width = query.shape
    head_size = qk_gain.shape[0]
    block = min(rows, 64)
    grad_query, contrib = pl.pallas_call(
        qk_kernel,
        grid=(rows // block,),
        in_specs=[
            pl.BlockSpec((block, width), lambda i: (i, 0)),
            pl.BlockSpec((block, width), lambda i: (i, 0)),
            pl.BlockSpec((1, head_size), lambda i: (0, 0)),
        ],
        out_specs=[
            pl.BlockSpec((block, width), lambda i: (i, 0)),
            pl.BlockSpec((8, head_size), lambda i: (0, 0)),
        ],
        out_shape=[
            jax.ShapeDtypeStruct((rows, width), jnp.bfloat16),
            jax.ShapeDtypeStruct((8, head_size), jnp.float32),
        ],
        compiler_params=pltpu.CompilerParams(vmem_limit_bytes=32 * 1024 * 1024),
        cost_estimate=pl.CostEstimate(flops=40 * rows * width, bytes_accessed=6 * rows * width, transcendentals=0),
    )(query, grad_normed, qk_gain.reshape(1, -1))
    return grad_query, jnp.sum(contrib, axis=0)


CORES = 2


def line_move(value, shift, valid):
    chips = lax.axis_size("dp") // CORES
    pairs = [
        (chip * CORES + core, (chip + shift) * CORES + core)
        for chip in range(chips)
        for core in range(CORES)
        if 0 <= chip + shift < chips and valid(chip)
    ]
    return lax.ppermute(value, "dp", pairs)


def partner_swap(value):
    count = lax.axis_size("dp")
    pairs = [(at, at - at % CORES + (at + 1) % CORES) for at in range(count)]
    return lax.ppermute(value, "dp", pairs)


def add_kernel(*refs):
    total = refs[0][...]
    for ref in refs[1:-1]:
        total = total + ref[...].astype(jnp.float32)
    refs[-1][...] = total.astype(jnp.bfloat16)


def add_terms(*terms):
    rows, width = terms[0].shape
    block = math.gcd(rows, 256)
    spec = pl.BlockSpec((block, width), lambda i: (i, 0))
    return pl.pallas_call(
        add_kernel,
        grid=(rows // block,),
        in_specs=[spec] * len(terms),
        out_specs=spec,
        out_shape=jax.ShapeDtypeStruct((rows, width), jnp.bfloat16),
        compiler_params=pltpu.CompilerParams(vmem_limit_bytes=16 * 1024 * 1024),
        cost_estimate=pl.CostEstimate(
            flops=3 * rows * width, bytes_accessed=10 * rows * width, transcendentals=0
        ),
    )(*terms)


def shards(block_input, prenorm_gain, weight, query, grad_normed, qk_gain):
    chips = lax.axis_size("dp") // CORES
    chip = lax.axis_index("dp") // CORES
    core = lax.axis_index("dp") % CORES
    columns = weight.shape[1]
    pair_columns = columns * CORES

    steps = []
    rightward, leftward = weight, weight
    for step in range(1, chips):
        rightward = line_move(rightward, 1, lambda at: at - step + 1 >= 0)
        leftward = line_move(leftward, -1, lambda at: at + step - 1 < chips)
        steps.append((rightward, leftward))

    input_wide_float = block_input.astype(jnp.float32)
    local_sum = jnp.sum(input_wide_float, axis=1)
    local_square = jnp.sum(input_wide_float * input_wide_float, axis=1)
    total_sum, total_square = lax.psum((local_sum, local_square), "mp")
    row_average = (total_sum / D)[:, None]
    reciprocal_deviation = lax.rsqrt((total_square / D)[:, None] - row_average * row_average + EPS)
    standardized_input = (input_wide_float - row_average) * reciprocal_deviation
    prenormed_rows = (standardized_input * prenorm_gain).astype(jnp.bfloat16)
    grad_query, qk_partial = qk_backward(query, grad_normed, qk_gain)

    def chip_columns(offset):
        first = lax.rem(chip + offset + chips, chips) * pair_columns
        return lax.dynamic_slice_in_dim(grad_query, first, pair_columns, 1)

    order = []
    for step in range(1, chips):
        for offset in ((chips - step) % chips, step):
            if offset not in order:
                order.append(offset)
    order.append(0)
    own, theirs = {}, {}
    for offset in order:
        part = lax.dot_general(
            prenormed_rows,
            chip_columns(offset),
            (((0,), (0,)), ((), ())),
            preferred_element_type=jnp.float32,
        )
        own[offset] = lax.dynamic_slice_in_dim(part, core * columns, columns, 1)
        theirs[offset] = partner_swap(
            lax.dynamic_slice_in_dim(part, (1 - core) * columns, columns, 1).astype(jnp.bfloat16)
        )

    to_right, to_left = None, None
    for step in range(1, chips):
        right_terms = [own[chips - step], theirs[chips - step]]
        left_terms = [own[step], theirs[step]]
        if step > 1:
            right_terms.append(to_right)
            left_terms.append(to_left)
        to_right = line_move(add_terms(*right_terms), 1, lambda at: at < step)
        to_left = line_move(add_terms(*left_terms), -1, lambda at: at >= chips - step)
    grad_weight = own[0] + theirs[0].astype(jnp.float32)
    if chips > 1:
        grad_weight = grad_weight + to_right.astype(jnp.float32) + to_left.astype(jnp.float32)

    def product(block, offset):
        other = partner_swap(block)
        first = jnp.where(core == 0, block, other)
        second = jnp.where(core == 0, other, block)
        return lax.dot_general(
            chip_columns(offset),
            jnp.concatenate([first, second], axis=1),
            (((1,), (1,)), ((), ())),
            preferred_element_type=jnp.float32,
        )

    gradient_prenormed_input = product(weight, 0)
    for step in range(1, chips):
        rightward, leftward = steps[step - 1]
        if 2 * step >= chips:
            from_left = chip >= step
            gradient_prenormed_input += product(
                jnp.where(from_left, rightward, leftward), jnp.where(from_left, -step, step)
            )
        else:
            gradient_prenormed_input += product(rightward, -step)
            gradient_prenormed_input += product(leftward, step)

    standardized_gradient = gradient_prenormed_input * prenorm_gain
    slope_mean, slope_cross = lax.psum(
        (
            jnp.sum(standardized_gradient, axis=1),
            jnp.sum(standardized_gradient * standardized_input, axis=1),
        ),
        "mp",
    )
    average_standardized_gradient = (slope_mean / D)[:, None]
    average_cross_term = (slope_cross / D)[:, None]
    input_gradient = (
        reciprocal_deviation
        * (
            standardized_gradient
            - average_standardized_gradient
            - standardized_input * average_cross_term
        )
    ).astype(jnp.bfloat16)
    prenorm_gain_partial = jnp.sum(gradient_prenormed_input * standardized_input, axis=0)
    prenorm_gain_gradient, grad_qk_gain = lax.psum((prenorm_gain_partial, qk_partial), "dp")
    return (input_gradient, grad_weight, prenorm_gain_gradient, grad_qk_gain)


def solution(mesh):
    return jax.shard_map(
        shards,
        mesh=mesh,
        in_specs=(P("dp", "mp"), P("mp"), P("mp", "dp"), P("dp", None), P("dp", None), P()),
        out_specs=(P("dp", "mp"), P("mp", "dp"), P("mp"), P()),
        check_vma=False,
    )
```
